32 devices in a mesh: row: 8 (over y, x, core), col: 4 (over z).
Axes of the slice: x: 2, y: 2, z: 4, core: 2. Of those that a mesh axis runs over, the one named last changes fastest.
Arguments:
- stiff_bb: bfloat16 [96, 3, 128, 384], P(('row', 'col')), may hold values from -6 to 6
- stiff_bi: bfloat16 [96, 384, 3072], P(('row', 'col')), may hold values from -6 to 6
- constraint_modes: bfloat16 [96, 3072, 384], P(('row', 'col')), may hold values from -0.109375 to 0.109375
- interior_mass: float32 [96, 3072], P(('row', 'col')), may hold values from 0.25 to 4
- fixed_modes: bfloat16 [96, 3072, 256], P(('row', 'col')), may hold values from -6 to 6
- mass_bb: bfloat16 [96, 3, 128, 384], P(('row', 'col')), may hold values from -6 to 6
- boundary_map: int32 [96, 3], P(('row', 'col')), may hold values from 0 to 191, as said below
Outputs:
- interface_stiffness: float32 [192, 4, 128, 128], P('row', None, 'col')
- interface_mass: float32 [192, 4, 128, 128], P('row', None, 'col')
- mass_coupling: float32 [96, 256, 384], P(('row', 'col'))
The draws below stay inside these ranges and needn't reach their ends.
Inputs may be any that keep to these rules, and one draw needn't show every extreme that they name: `boundary_map`: row s holds blocks b, b + a, b + c with 0 < a < c < 4, all three in the range of one owner (block // 24). Rows come in aligned row groups of 12; no owner serves more than 2 rows of one row group, and in every draw one owner serves exactly 2 rows of every row group.
All inputs are finite; a program needn't handle non-finite values.
Results may differ from the reference program's by a relative error of at most 0.0029.
Values sent between devices are 32-bit elements; how exact they have to be, the bound alone decides.
A program may use at most 192 MiB of HBM per device.

```python
import math
import jax
import jax.numpy as jnp
from jax import lax

NI = 3072
BLK = 128
NB = 384
NM = 256
BAND = 4
BPO = 24
SE_GRP = 12
CAP = 2
SETOT = 96
NBLOCK = 192
N_ROW = 8


def draw_boundary_map(key, part):
    slot_count = N_ROW * CAP
    keys = jax.random.split(jax.random.fold_in(key, 17), 7)
    priority_tiers = jax.random.randint(keys[0], (N_ROW,), 0, 4)
    busiest_targets = jax.random.randint(keys[1], (), 0, N_ROW)
    position_owner = jnp.arange(slot_count) // CAP
    random_jitter = jax.random.randint(keys[2], (N_ROW, slot_count), 0, 65536)
    extra_credit = jnp.where(position_owner == busiest_targets, 1 << 20, 0)
    ranking_values = random_jitter + priority_tiers[position_owner][None, :] * 16384 + extra_credit[None, :]
    ranking_values = ranking_values * slot_count + jnp.arange(slot_count)[None, :]
    picked = lax.top_k(ranking_values, SE_GRP)[1]
    order_scores = jax.random.randint(keys[3], (N_ROW, SE_GRP), 0, 4096) * SE_GRP + jnp.arange(SE_GRP)[None, :]
    order = lax.top_k(order_scores, SE_GRP)[1]
    picked = jnp.take_along_axis(picked, order, axis=1)
    owners = (picked // CAP).reshape(SETOT)
    first = jax.random.randint(keys[4], (SETOT,), 1, BAND - 1)
    second = first + jax.random.randint(keys[5], (SETOT,), 1, BAND - first)
    start = owners * BPO + jax.random.randint(keys[6], (SETOT,), 0, BPO - second)
    return jnp.stack([start, start + first, start + second], axis=1).astype(jnp.int32)


def steps_of(rng, extent, cuts, low, top_value):
    gain, own = 1.0, jax.random.fold_in(rng, 6)
    for position, blocks in cuts:
        steps = jnp.exp(jax.random.uniform(jax.random.fold_in(own, position), (blocks,), jnp.float32, low / len(cuts), top_value / len(cuts)))
        gain = gain * jnp.repeat(steps, extent[position] // blocks).reshape([-1 if axis == position else 1 for axis in range(len(extent))])
    return gain


def centred(key, extent, deviation, most, pieces=(), dtype=jnp.bfloat16):
    array = deviation * jax.random.normal(key, extent, jnp.float32)
    if pieces:
        array = array * steps_of(key, extent, pieces, -0.22, 0.18)
    return jnp.clip(array, -most, most).astype(dtype)


def setup_inputs(seed: int = 0) -> dict:
    streams_of = jax.random.split(jax.random.key(seed), 8)
    return {
        "stiff_bb": centred(streams_of[0], (SETOT, 3, BLK, NB), 1.0, 6.0, ((0, 32),)),
        "stiff_bi": centred(streams_of[1], (SETOT, NB, NI), 1.0, 6.0, ((0, 32),)),
        "constraint_modes": centred(streams_of[2], (SETOT, NI, NB), NI ** -0.5, 0.109375, ((0, 32),)),
        "interior_mass": jnp.clip(jnp.exp(math.log(4.0) - 2.7725887 * jax.random.uniform(streams_of[3], (SETOT, NI), jnp.float32) ** steps_of(streams_of[3], (SETOT, NI), ((0, 32),), -0.2, 0.2)), 0.25, 4.0),
        "fixed_modes": centred(streams_of[4], (SETOT, NI, NM), 1.0, 6.0, ((0, 32),)),
        "mass_bb": centred(streams_of[5], (SETOT, 3, BLK, NB), 1.0, 6.0, ((0, 32),)),
        "boundary_map": draw_boundary_map(jax.random.fold_in(streams_of[7], 71), 0),
    }


PAIRS = ((0, 0), (1, 1), (2, 2), (0, 1), (0, 2), (1, 2))


def reduce_one(items):
    block_bb, block_bi, psi, masses, modes, mass_block = items
    order = block_bi.shape[0]
    weighted = (masses[:, None] * psi.astype(jnp.float32)).astype(jnp.bfloat16)
    red_k = block_bb.reshape(order, order).astype(jnp.float32) + jnp.dot(block_bi, psi, preferred_element_type=jnp.float32)
    red_m = mass_block.reshape(order, order).astype(jnp.float32) + jnp.dot(psi.T, weighted, preferred_element_type=jnp.float32)
    coupling = jnp.dot(modes.T, weighted, preferred_element_type=jnp.float32)
    return red_k, red_m, coupling


def reference(stiff_bb, stiff_bi, constraint_modes, interior_mass, fixed_modes, mass_bb, boundary_map):
    red_k, red_m, coupling = lax.map(reduce_one, (stiff_bb, stiff_bi, constraint_modes, interior_mass, fixed_modes, mass_bb))
    width = stiff_bb.shape[2]
    total_k = jnp.zeros((NBLOCK, BAND, width, width), jnp.float32)
    total_m = jnp.zeros((NBLOCK, BAND, width, width), jnp.float32)
    for first, second in PAIRS:
        rows = boundary_map[:, first].astype(jnp.int32)
        offset = (boundary_map[:, second] - boundary_map[:, first]).astype(jnp.int32)
        piece_k = red_k[:, first * width:(first + 1) * width, second * width:(second + 1) * width]
        piece_m = red_m[:, first * width:(first + 1) * width, second * width:(second + 1) * width]
        total_k = total_k.at[rows, offset].add(piece_k)
        total_m = total_m.at[rows, offset].add(piece_m)
    return total_k, total_m, coupling
```

```python
import functools
import jax
import jax.numpy as jnp
from jax import lax
from jax.experimental import pallas as pl
from jax.experimental.pallas import tpu as pltpu
from jax.sharding import PartitionSpec as P

BAND = 4
BPO = 24
LANE = 128

PAIRS = ((0, 0), (1, 1), (2, 2), (0, 1), (0, 2), (1, 2))
KINDS = 2
CHUNKS = KINDS * len(PAIRS)
MESH = pl.DeviceIdType.MESH
VMEM_LIMIT = 60 * 1024 * 1024


def at_col(z):
    return {"row": lax.axis_index("row"), "col": z}


def at_row(r):
    return {"row": r, "col": lax.axis_index("col")}


def reduce_and_send(
    owners, lanes, slots,
    kbb, kbi, psi, mass, modes, mbb, table,
    got, all_maps, coupling,
    kbb_v, kbi_v, psi_v, modes_v, mbb_v, weighted, coupled, product,
    reduced, grouped, staging, outgoing, maps_v, maps_s,
    in_sems, z_send, z_recv, r_send, r_recv, r_own,
    zm_send, zm_recv, rm_send, rm_recv, small, out_sems,
):
    count, order, inner = kbi.shape
    width = order // 3
    part = width // lanes
    members = count * lanes
    row = lax.axis_index("row")
    col = lax.axis_index("col")

    def loads(s):
        return (
            pltpu.make_async_copy(kbi.at[s], kbi_v.at[s], in_sems.at[0, s]),
            pltpu.make_async_copy(psi.at[s], psi_v.at[s], in_sems.at[1, s]),
            pltpu.make_async_copy(kbb.at[s], kbb_v.at[s], in_sems.at[2, s]),
        )

    def late_loads(s):
        return (
            pltpu.make_async_copy(mbb.at[s], mbb_v.at[s], in_sems.at[3, s]),
            pltpu.make_async_copy(modes.at[s], modes_v.at[s], in_sems.at[4, s]),
        )

    for s in range(count):
        for copy in loads(s):
            copy.start()
    for s in range(count):
        for copy in late_loads(s):
            copy.start()

    barrier = pltpu.get_barrier_semaphore()
    for i in range(1, lanes):
        pl.semaphore_signal(barrier, inc=1, device_id=at_col(lax.rem(col + i, lanes)), device_id_type=MESH)

    def greet(i, carry):
        pl.semaphore_signal(barrier, inc=1, device_id=at_row(lax.rem(row + i, owners)), device_id_type=MESH)
        return carry

    lax.fori_loop(1, owners, greet, 0)

    def put(kind, s, total):
        for p, (i, j) in enumerate(PAIRS):
            block = total[i * width : (i + 1) * width, j * width : (j + 1) * width]
            reduced[kind * len(PAIRS) + p, :, s] = block.reshape(lanes, part, width)

    def stiffness(s, carry):
        for copy in loads(s):
            copy.wait()
        product[...] = jnp.dot(kbi_v[s], psi_v[s], preferred_element_type=jnp.float32)
        put(0, s, product[...] + kbb_v[s].astype(jnp.float32).reshape(order, order))
        return carry

    lax.fori_loop(0, count, stiffness, 0)
    pl.semaphore_wait(barrier, lanes - 1 + owners - 1)

    def z_map(i):
        return pltpu.make_async_remote_copy(
            src_ref=table, dst_ref=maps_v.at[col],
            send_sem=zm_send.at[i], recv_sem=zm_recv.at[lanes - i],
            device_id=at_col(lax.rem(col + i, lanes)), device_id_type=MESH,
        )

    def z_copy(p, i):
        to = lax.rem(col + i, lanes)
        return pltpu.make_async_remote_copy(
            src_ref=reduced.at[p, to], dst_ref=grouped.at[p, col],
            send_sem=z_send.at[p, i], recv_sem=z_recv.at[p, lanes - i],
            device_id=at_col(to), device_id_type=MESH,
        )

    for i in range(1, lanes):
        z_map(i).start()
    maps_v[col] = table[...]

    half = len(PAIRS)

    def send_chunk(p, carry):
        for i in range(1, lanes):
            z_copy(p, i).start()
        grouped[p, col] = reduced[p, col]
        return carry

    lax.fori_loop(0, half, send_chunk, 0)

    def masses(s, carry):
        for copy in late_loads(s):
            copy.wait()

        def weigh(k, inner_carry):
            start = pl.multiple_of(k * LANE, LANE)
            lines = mass[:, pl.ds(start, LANE)]
            chosen = lax.broadcasted_iota(jnp.int32, lines.shape, 0) == s
            line = jnp.sum(jnp.where(chosen, lines, 0.0), axis=0, keepdims=True)
            column = jnp.broadcast_to(line, (LANE, LANE)).T
            scale = jnp.concatenate([column] * (order // LANE), axis=1)
            values = psi_v[s, pl.ds(start, LANE), :].astype(jnp.float32)
            weighted[pl.ds(start, LANE), :] = (scale * values).astype(jnp.bfloat16)
            return inner_carry

        lax.fori_loop(0, inner // LANE, weigh, 0)
        across = (((0,), (0,)), ((), ()))
        product[...] = lax.dot_general(psi_v[s], weighted[...], across, preferred_element_type=jnp.float32)
        put(1, s, product[...] + mbb_v[s].astype(jnp.float32).reshape(order, order))
        coupled[s] = lax.dot_general(modes_v[s], weighted[...], across, preferred_element_type=jnp.float32)
        pltpu.make_async_copy(coupled.at[s], coupling.at[s], out_sems.at[s]).start()
        return carry

    lax.fori_loop(0, count, masses, 0)
    lax.fori_loop(half, CHUNKS, send_chunk, 0)

    for i in range(1, lanes):
        z_map(i).wait()
    to_scalar = pltpu.make_async_copy(maps_v, maps_s, small.at[0])
    to_scalar.start()

    def r_map(i):
        return pltpu.make_async_remote_copy(
            src_ref=maps_v, dst_ref=all_maps.at[row],
            send_sem=rm_send.at[i], recv_sem=rm_recv.at[owners - i],
            device_id=at_row(lax.rem(row + i, owners)), device_id_type=MESH,
        )

    lax.fori_loop(1, owners, lambda i, c: (r_map(i).start(), c)[1], 0)
    own_map = pltpu.make_async_copy(maps_v, all_maps.at[row], small.at[1])
    own_map.start()
    to_scalar.wait()

    belongs = [maps_s[m // count, 0, 3 * (m % count)] // BPO for m in range(members)]
    ranks = []
    for m in range(members):
        rank = jnp.int32(0)
        for e in range(m):
            rank = rank + jnp.where(belongs[e] == belongs[m], 1, 0)
        ranks.append(rank)
    places = [belongs[m] * slots + ranks[m] for m in range(members)]

    chosen = []
    for slot in range(owners * slots):
        member = jnp.int32(0)
        for m in range(1, members):
            member = jnp.where(places[m] == slot, m, member)
        chosen.append(member)

    def forward(p, carry):
        for i in range(1, lanes):
            z_copy(p, i).wait_recv()

        staging[...] = grouped[p].reshape(members, part, width)
        for slot, member in enumerate(chosen):
            outgoing[p, slot // slots, slot % slots] = staging[member]

        def ship(i, inner_carry):
            r_copy(p, i).start()
            return inner_carry

        lax.fori_loop(1, owners, ship, 0)
        own_copy(p).start()
        return carry

    def r_copy(p, i):
        to = lax.rem(row + i, owners)
        return pltpu.make_async_remote_copy(
            src_ref=outgoing.at[p, to], dst_ref=got.at[p, row],
            send_sem=r_send.at[p], recv_sem=r_recv.at[p],
            device_id=at_row(to), device_id_type=MESH,
        )

    def own_copy(p):
        return pltpu.make_async_copy(outgoing.at[p, row], got.at[p, row], r_own.at[p])

    lax.fori_loop(0, CHUNKS, forward, 0)

    def settle(p, carry):
        for i in range(1, lanes):
            z_copy(p, i).wait_send()
        rest = got.at[p, pl.ds(0, owners - 1)]
        pltpu.make_async_copy(rest, rest, r_send.at[p]).wait()
        pltpu.make_async_copy(rest, rest, r_recv.at[p]).wait()
        own_copy(p).wait()
        return carry

    lax.fori_loop(0, CHUNKS, settle, 0)
    lax.fori_loop(1, owners, lambda i, c: (r_map(i).wait(), c)[1], 0)
    own_map.wait()
    for s in range(count):
        pltpu.make_async_copy(coupled.at[s], coupling.at[s], out_sems.at[s]).wait()


def assemble(owners, lanes, count, slots, got, all_maps, k_out, m_out, buffer, maps_s, sems, small):
    to_scalar = pltpu.make_async_copy(all_maps.at[:, :, pl.ds(0, 1)], maps_s, small.at[0])
    to_scalar.start()
    for p in range(CHUNKS):
        pltpu.make_async_copy(got.at[p], buffer.at[p], sems.at[p]).start()
    k_out[...] = jnp.zeros_like(k_out)
    m_out[...] = jnp.zeros_like(m_out)
    to_scalar.wait()
    for p in range(CHUNKS):
        pltpu.make_async_copy(got.at[p], buffer.at[p], sems.at[p]).wait()
    me = lax.axis_index("row")
    first = me * BPO

    def per_group(group, carry):
        def per_member(m, filled):
            z, s = m // count, m % count
            blocks = [maps_s[group, z, 0, 3 * s + k] for k in range(3)]
            mine = blocks[0] // BPO == me

            @pl.when(mine)
            def _():
                for p, (i, j) in enumerate(PAIRS):
                    at, offset = blocks[i] - first, blocks[j] - blocks[i]
                    k_out[at, offset] += buffer[p, group, filled]
                    m_out[at, offset] += buffer[len(PAIRS) + p, group, filled]

            return filled + jnp.where(mine, 1, 0)

        lax.fori_loop(0, count * lanes, per_member, jnp.int32(0))
        return carry

    lax.fori_loop(0, owners, per_group, 0)


def per_device(
    stiff_bb, stiff_bi, constraint_modes, interior_mass, fixed_modes, mass_bb, boundary_map
):
    owners = lax.axis_size("row")
    lanes = lax.axis_size("col")
    count, order, inner = stiff_bi.shape
    modes = fixed_modes.shape[2]
    width = order // 3
    part = width // lanes
    slots = (count * lanes + owners - 1) // owners
    f32, bf16 = jnp.float32, jnp.bfloat16
    table = jnp.pad(boundary_map.reshape(1, count * 3), ((0, 7), (0, LANE - count * 3)))
    hbm = pl.BlockSpec(memory_space=pl.ANY)
    vmem = pl.BlockSpec(memory_space=pltpu.VMEM)
    dma = pltpu.SemaphoreType.DMA
    got, all_maps, coupling = pl.pallas_call(
        functools.partial(reduce_and_send, owners, lanes, slots),
        out_shape=(
            jax.ShapeDtypeStruct((CHUNKS, owners, slots, part, width), f32),
            jax.ShapeDtypeStruct((owners, lanes, 8, LANE), jnp.int32),
            jax.ShapeDtypeStruct((count, modes, order), f32),
        ),
        in_specs=[hbm, hbm, hbm, vmem, hbm, hbm, vmem],
        out_specs=(hbm, hbm, hbm),
        scratch_shapes=[
            pltpu.VMEM((count, 3, width, order), bf16),
            pltpu.VMEM((count, order, inner), bf16),
            pltpu.VMEM((count, inner, order), bf16),
            pltpu.VMEM((count, inner, modes), bf16),
            pltpu.VMEM((count, 3, width, order), bf16),
            pltpu.VMEM((inner, order), bf16),
            pltpu.VMEM((count, modes, order), f32),
            pltpu.VMEM((order, order), f32),
            pltpu.VMEM((CHUNKS, lanes, count, part, width), f32),
            pltpu.VMEM((CHUNKS, lanes, count, part, width), f32),
            pltpu.VMEM((lanes * count, part, width), f32),
            pltpu.VMEM((CHUNKS, owners, slots, part, width), f32),
            pltpu.VMEM((lanes, 8, LANE), jnp.int32),
            pltpu.SMEM((lanes, 8, LANE), jnp.int32),
            dma((5, count)),
            dma((CHUNKS, lanes)),
            dma((CHUNKS, lanes)),
            dma((CHUNKS,)),
            dma((CHUNKS,)),
            dma((CHUNKS,)),
            dma((lanes,)),
            dma((lanes,)),
            dma((owners,)),
            dma((owners,)),
            dma((2,)),
            dma((count,)),
        ],
        compiler_params=pltpu.CompilerParams(
            collective_id=0, has_side_effects=True, vmem_limit_bytes=VMEM_LIMIT
        ),
        name="reduce_and_send",
    )(stiff_bb, stiff_bi, constraint_modes, interior_mass, fixed_modes, mass_bb, table)
    block = jax.ShapeDtypeStruct((BPO, BAND, part, width), f32)
    k_out, m_out = pl.pallas_call(
        functools.partial(assemble, owners, lanes, count, slots),
        out_shape=(block, block),
        in_specs=[hbm, hbm],
        out_specs=(vmem, vmem),
        scratch_shapes=[
            pltpu.VMEM(got.shape, f32),
            pltpu.SMEM((owners, lanes, 1, LANE), jnp.int32),
            dma((CHUNKS,)),
            dma((1,)),
        ],
        compiler_params=pltpu.CompilerParams(vmem_limit_bytes=VMEM_LIMIT),
        name="assemble",
    )(got, all_maps)
    return k_out, m_out, coupling


def solution(mesh):
    placed = (
        P(("row", "col"), None, None, None),
        P(("row", "col"), None, None),
        P(("row", "col"), None, None),
        P(("row", "col"), None),
        P(("row", "col"), None, None),
        P(("row", "col"), None, None, None),
        P(("row", "col"), None),
    )
    return jax.shard_map(
        per_device,
        mesh=mesh,
        in_specs=placed,
        out_specs=(
            P("row", None, "col", None),
            P("row", None, "col", None),
            P(("row", "col"), None, None),
        ),
        check_vma=False,
    )
```
